128 devices in a mesh: seg: 128 (over y, x, z, core).
Axes of the slice: x: 4, y: 4, z: 4, core: 2. Of those that a mesh axis runs over, the one named last changes fastest.
Arguments:
- strain: bfloat16 [3, 256, 3, 2, 65536], P(None, 'seg'), may hold values from -6 to 6
- valid: int32 [256], P('seg'), may hold values from 0 to 1, as said below
- intersection: float32 [3, 65536], replicated, may hold values from -1 to 1, as said below
- notch: int32 [65536], replicated, may hold values from 0 to 1, as said below
Outputs:
- contribution: float32 [3, 65536], P(None, 'seg')
- broadband: float32 [3, 2], replicated
The draws below stay inside these ranges and needn't reach their ends.
Inputs may be any that keep to these rules, and one draw needn't show every extreme that they name: At least one segment is valid. `intersection`: never zero. `notch`: at least one bin is kept.
All inputs are finite; a program needn't handle non-finite values.
Results may differ from the reference program's by a relative error of at most 0.011.
Values sent between devices are 32-bit elements; how exact they have to be, the bound alone decides.
A program may use at most 256 MiB of HBM per device.

```python
import math
import jax
import jax.numpy as jnp
from jax import lax

FA = 256
FB = 256
STR = 3
SEGMENTS = 256


def draw_valid(key, part):
    marks = jax.random.randint(jax.random.fold_in(key, 11), (SEGMENTS,), 0, 4)
    forced = jax.random.randint(jax.random.fold_in(key, 12), (), 0, SEGMENTS)
    flags = jnp.where(marks > 0, 1, 0)
    flags = jnp.where(jnp.arange(SEGMENTS) == forced, 1, flags)
    return flags.astype(jnp.int32)


def draw_notch(key, part):
    marks = jax.random.randint(jax.random.fold_in(key, 21), (FA * FB,), 0, 10)
    forced = jax.random.randint(jax.random.fold_in(key, 22), (), 0, FA * FB)
    flags = jnp.where(marks > 0, 1, 0)
    flags = jnp.where(jnp.arange(FA * FB) == forced, 1, flags)
    return flags.astype(jnp.int32)


def draw_intersection(key, part):
    position = jnp.arange(FA * FB, dtype=jnp.float32)[None, :] / (FA * FB)
    signs = jax.random.randint(jax.random.fold_in(key, 31), (3, FA * FB), 0, 2)
    signs = jnp.where(signs > 0, 1.0, -1.0)
    rough = jax.random.uniform(jax.random.fold_in(key, 33), (3, FA * FB), jnp.float32, 0.3, 1.0)
    shape = jnp.exp(-1.5 * position)
    return (signs * rough * shape).astype(jnp.float32)


def block_scale(key, shape, shards, low, high):
    def one(dim, parts):
        steps = jax.random.uniform(jax.random.fold_in(jax.random.fold_in(key, 6), dim), (parts,), jnp.float32, low / len(shards), high / len(shards))
        return jnp.repeat(jnp.exp(steps), shape[dim] // parts).reshape((-1,) + (1,) * (len(shape) - dim - 1))

    loudness = one(*shards[0])
    for cut in shards[1:]:
        loudness = loudness * one(*cut)
    return loudness


def normal_values(stream_key, shape, width, bound, shards=(), kind=jnp.bfloat16):
    drawn = width * jax.random.normal(stream_key, shape, jnp.float32)
    if shards:
        drawn = drawn * block_scale(stream_key, shape, shards, -0.22, 0.18)
    return jnp.clip(drawn, -bound, bound).astype(kind)


def setup_inputs(seed: int = 0) -> dict:
    key_of = jax.random.split(jax.random.key(seed), 5)
    return {
        "strain": normal_values(key_of[0], (3, SEGMENTS, STR, 2, FA * FB), 1.0, 6.0, ((1, 128),)),
        "valid": draw_valid(jax.random.fold_in(key_of[4], 71), 0),
        "intersection": draw_intersection(jax.random.fold_in(key_of[4], 71), 0),
        "notch": draw_notch(jax.random.fold_in(key_of[4], 71), 0),
    }


baseline_pairs = ((0, 1), (0, 2), (1, 2))

def dft_tables(length):
    counter = jnp.arange(length, dtype=jnp.int32)
    phases = counter[:, None] * counter[None, :] % length
    angles = phases.astype(jnp.float32) * (2.0 * math.pi / length)
    return (jnp.cos(angles).astype(jnp.bfloat16), jnp.sin(angles).astype(jnp.bfloat16))

def twiddle(rows, cols):
    phases = jnp.arange(rows, dtype=jnp.int32)[:, None] * jnp.arange(cols, dtype=jnp.int32)[None, :]
    angles = phases.astype(jnp.float32) * (2.0 * math.pi / (rows * cols))
    return (jnp.cos(angles), jnp.sin(angles))

def mult(table, data, form):
    return jnp.einsum(form, table.astype(jnp.float32), data.astype(jnp.float32))

def spectra(strain, rows, cols):
    lead = strain.shape[:3]
    real_in = strain[:, :, :, 0].reshape(-1, rows, cols)
    imag_in = strain[:, :, :, 1].reshape(-1, rows, cols)
    cos_rows, sin_rows = dft_tables(rows)
    first_real = mult(cos_rows, real_in, 'kn,bnq->bkq') + mult(sin_rows, imag_in, 'kn,bnq->bkq')
    first_imag = mult(cos_rows, imag_in, 'kn,bnq->bkq') - mult(sin_rows, real_in, 'kn,bnq->bkq')
    tw_cos, tw_sin = twiddle(rows, cols)
    mid_real = (first_real * tw_cos + first_imag * tw_sin).astype(jnp.bfloat16)
    mid_imag = (first_imag * tw_cos - first_real * tw_sin).astype(jnp.bfloat16)
    cos_cols, sin_cols = dft_tables(cols)
    last_real = mult(cos_cols, mid_real, 'kn,bpn->bkp') + mult(sin_cols, mid_imag, 'kn,bpn->bkp')
    last_imag = mult(cos_cols, mid_imag, 'kn,bpn->bkp') - mult(sin_cols, mid_real, 'kn,bpn->bkp')
    scale = 1.0 / math.sqrt(rows * cols)
    shape = lead + (rows * cols,)
    return (last_real.reshape(shape) * scale, last_imag.reshape(shape) * scale)

def segment_stats(real_part, imag_part, valid_float):
    power = lax.optimization_barrier(jnp.mean(real_part * real_part + imag_part * imag_part, axis=2))
    weights = []
    weighted = []
    for first, second in baseline_pairs:
        cross = lax.optimization_barrier(jnp.mean(real_part[first] * real_part[second] + imag_part[first] * imag_part[second], axis=1))
        weight = valid_float[:, None] / (power[first] * power[second])
        weights.append(weight)
        weighted.append(weight * cross)
    return jnp.stack(weights + weighted, axis=1)

def reference(strain, valid, intersection, notch):

    def step(carry, index):
        piece = lax.dynamic_slice_in_dim(strain, index, 1, 1)
        flags = lax.dynamic_slice_in_dim(valid, index, 1, 0).astype(jnp.float32)
        real_part, imag_part = spectra(piece, FA, FB)
        return (carry + segment_stats(real_part, imag_part, flags)[0], None)
    start = jnp.zeros((6, FA * FB), jnp.float32)
    sums, _ = lax.scan(step, start, jnp.arange(SEGMENTS, dtype=jnp.int32))
    weight_sum = sums[:3]
    numer = sums[3:]
    kept = notch.astype(jnp.float32)[None, :]
    signal = lax.optimization_barrier(jnp.sum(kept * intersection * numer, axis=1))
    info = lax.optimization_barrier(jnp.sum(kept * intersection * intersection * weight_sum, axis=1))
    contribution = kept * intersection * numer / jnp.sqrt(info / (FA * FB))[:, None]
    broadband = jnp.stack([signal / jnp.sqrt(info), jnp.sqrt(info / (FA * FB))], axis=1)
    return (contribution, broadband)
```

```python
import functools
import math

import jax
import jax.numpy as jnp
import numpy as np
from jax import lax
from jax.experimental import pallas as pl
from jax.experimental.pallas import tpu as pltpu
from jax.sharding import PartitionSpec as P

MESH = pl.DeviceIdType.MESH
F = 256
BINS = F * F
CHIPS = 64
PAIRS = ((0, 1), (0, 2), (1, 2))
ROWS = 64
f32, bf16 = jnp.float32, jnp.bfloat16


def tables():
    k = np.arange(F)
    angle = 2 * np.pi * ((k[:, None] * k[None, :]) % F) / F
    cos, sin = (t(angle).astype(bf16).astype(np.float32) for t in (np.cos, np.sin))
    s = np.arange(8)
    a_of = (8 * np.arange(32)[:, None] + (s // 2 + 4 * (s % 2))[None, :]).reshape(-1)
    one = np.zeros((2, F, F, 2), np.float32)
    one[0, :, :, 0], one[0, :, :, 1] = cos[:, a_of], sin[:, a_of]
    one[1, :, :, 0], one[1, :, :, 1] = -sin[:, a_of], cos[:, a_of]
    one = one.reshape(2, 16, 16, 512).transpose(1, 0, 2, 3).reshape(512, 512)
    one = one.reshape(512, 4, 128).transpose(1, 0, 2)
    w, r, chip = np.meshgrid(np.arange(2), np.arange(2), np.arange(CHIPS), indexing="ij")
    q_of = (4 * chip + 2 * w + r).reshape(-1)
    c, v = cos[:, q_of] / F, sin[:, q_of] / F
    two = np.block([[c, -v], [v, c]])
    two = two.reshape(512, 4, 128).transpose(1, 0, 2)
    turn = 2 * np.pi * (k[:, None] * k[None, :]) / BINS
    turns = np.stack([np.cos(turn), np.sin(turn)]).astype(np.float32)
    return one.astype(bf16), two.astype(bf16), turns


def kernel(valid, strain, inter, notch, one, two, turns, out, board,
           x, l1, l2, uv, it, nt, at, mid, y, part, num, came, send, recv, sc, sccame,
           load_sem, x_sem, pair_sem, out_sem, in_sem):
    me = lax.axis_index("seg")
    chip, core = me // 2, lax.rem(me, 2)
    mate = me + 1 - 2 * core

    loads = [pltpu.make_async_copy(a, b, load_sem.at[n]) for n, (a, b) in enumerate(
        ((inter, it.at[:, :3]), (notch, nt), (one, l1), (turns, uv), (two, l2)))]
    takes = [pltpu.make_async_copy(strain.at[n], x.at[n], x_sem.at[n]) for n in range(18)]
    for c in loads[:4] + takes + loads[4:]:
        c.start()

    barrier = pltpu.get_barrier_semaphore()
    pl.semaphore_signal(barrier, inc=1, device_id=(mate,), device_id_type=MESH)

    @pl.loop(1, CHIPS)
    def _(r):
        to = lax.rem(chip + r, CHIPS) * 2 + core
        pl.semaphore_signal(barrier, inc=1, device_id=(to,), device_id_type=MESH)

    loads[0].wait()
    loads[1].wait()
    rows4 = it.reshape(2048, 128)
    for h in range(2):
        for w in range(2):
            keep = [nt[pl.ds(2 * (2 * w + r) + h, CHIPS, stride=8), :].astype(f32) for r in range(2)]
            for i in range(3):
                got = [rows4[pl.ds(8 * (2 * w + r) + 4 * h + i, CHIPS, stride=32), :] * keep[r] for r in range(2)]
                at[i, h, :, w * 128:(w + 1) * 128] = jnp.concatenate(got, axis=0).T

    even = (lax.broadcasted_iota(jnp.int16, (16, 128), 0) & 2) == 0
    loads[2].wait()
    loads[3].wait()
    for n in range(18):
        takes[n].wait()
        left, right = [], []
        for g in range(32):
            a, b = x[n, pl.ds(32 * g, 16), :], x[n, pl.ds(32 * g + 16, 16), :]
            left.append(jnp.where(even, a, pltpu.roll(b, 2, axis=0)))
            right.append(jnp.where(even, pltpu.roll(a, 14, axis=0), b))
        data = jnp.concatenate([jnp.concatenate(left, 0), jnp.concatenate(right, 0)], axis=1)
        table = jnp.concatenate([l1[k] for k in range(4)], axis=1)
        first = jnp.dot(table, data, preferred_element_type=f32)
        for g in range(16):
            re, im = first[32 * g:32 * g + 16], first[32 * g + 16:32 * g + 32]
            u, v = uv[0, pl.ds(16 * g, 16), :], uv[1, pl.ds(16 * g, 16), :]
            mr = (re * u + im * v).astype(bf16)
            mi = (im * u - re * v).astype(bf16)
            for h in range(2):
                mid[n, h, pl.ds(16 * g, 16), :] = mr[:, 128 * h:128 * h + 128]
                mid[n, 2 + h, pl.ds(16 * g, 16), :] = mi[:, 128 * h:128 * h + 128]

    loads[4].wait()
    pl.semaphore_wait(barrier, CHIPS)

    def second(block, s, slot):
        rows = pl.ds(ROWS * block, ROWS)
        which = [d * 6 + s * 3 + t for t in range(3) for d in range(3)]
        data = jnp.concatenate(
            [jnp.concatenate([mid[n, k, rows, :] for n in which], axis=0) for k in range(4)], axis=1)
        table = jnp.concatenate([l2[k] for k in range(4)], axis=1)
        y[slot] = jnp.dot(data, table, preferred_element_type=f32)

    signal = [jnp.zeros((8, 128), f32)] * 3
    info = [jnp.zeros((8, 128), f32)] * 3

    def stats(block, s, slot):
        ok = valid[s].astype(f32)
        for g in range(ROWS // 8):
            for w in range(2):
                lane = slice(128 * w, 128 * w + 128)
                lane_im = slice(256 + 128 * w, 384 + 128 * w)
                power = [None] * 3
                cross = [None] * 3
                for t in range(3):
                    at_row = lambda d: pl.ds(ROWS * (3 * t + d) + 8 * g, 8)
                    re = [y[slot, at_row(d), lane] for d in range(3)]
                    im = [y[slot, at_row(d), lane_im] for d in range(3)]
                    for d in range(3):
                        v = re[d] * re[d] + im[d] * im[d]
                        power[d] = v if t == 0 else power[d] + v
                    for i, (a, b) in enumerate(PAIRS):
                        v = re[a] * re[b] + im[a] * im[b]
                        cross[i] = v if t == 0 else cross[i] + v
                third = [p * (1.0 / 3.0) for p in power]
                half, row = divmod(ROWS * block + 8 * g, 128)
                row = pl.ds(row, 8)
                for i, (a, b) in enumerate(PAIRS):
                    weight = ok / (third[a] * third[b])
                    v = weight * (cross[i] * (1.0 / 3.0))
                    f = at[i, half, row, lane]
                    signal[i] = signal[i] + f * v
                    info[i] = info[i] + f * f * weight
                    if s == 0:
                        part[i, half, row, lane] = v
                    else:
                        part[i, half, row, lane] = part[i, half, row, lane] + v

    def pair(half):
        return pltpu.make_async_remote_copy(
            src_ref=num.at[half, 1 - core], dst_ref=came.at[half],
            send_sem=pair_sem.at[half], recv_sem=pair_sem.at[2 + half],
            device_id=(mate,), device_id_type=MESH)

    def turn(half):
        for w in range(2):
            for i in range(3):
                num[half, w, i] = part[i, half, :, w * 128:(w + 1) * 128].T

    def merge(half):
        for i in range(3):
            for r in range(2):
                send[half, pl.ds(2 * i + r, CHIPS, stride=8), :] = (
                    num[half, core, i, pl.ds(CHIPS * r, CHIPS), :] + came[half, i, pl.ds(CHIPS * r, CHIPS), :])

    def spread(half):
        @pl.loop(1, CHIPS)
        def _(r):
            to = lax.rem(chip + r, CHIPS)
            pltpu.make_async_remote_copy(
                src_ref=send.at[half, pl.ds(pl.multiple_of(8 * to, 8), 8)],
                dst_ref=recv.at[half, pl.ds(pl.multiple_of(8 * (r - 1), 8), 8)],
                send_sem=out_sem.at[half], recv_sem=in_sem.at[half],
                device_id=(2 * to + core,), device_id_type=MESH).start()

    order = [(block, s) for block in range(F // ROWS) for s in range(2)]
    for n, (block, s) in enumerate(order):
        second(block, s, n % 2)
        if n:
            stats(*order[n - 1], (n - 1) % 2)
        if n == 5:
            turn(0)
            pair(0).start()
    stats(*order[-1], 1)
    turn(1)
    rows = [jnp.sum(a, axis=0, keepdims=True) for a in signal + info]
    cells = [jnp.sum(a, axis=1, keepdims=True) for a in rows]
    lanes = lax.broadcasted_iota(jnp.int32, (1, 128), 1)
    lines = []
    for group in (cells[:3], cells[3:]):
        line = jnp.zeros((1, 128), f32)
        for i in range(3):
            line = jnp.where(lanes == i, group[i], line)
        lines.append(line)
    sc[...] = jnp.concatenate(lines + [jnp.zeros((6, 128), f32)], axis=0)
    scalars = pltpu.make_async_remote_copy(
        src_ref=sc, dst_ref=sccame, send_sem=pair_sem.at[4], recv_sem=pair_sem.at[5],
        device_id=(mate,), device_id_type=MESH)
    pair(1).start()
    scalars.start()
    pair(0).wait()
    for r in range(2):
        send[0, pl.ds(6 + r, CHIPS, stride=8), :] = jnp.zeros((CHIPS, 128), f32)
    merge(0)
    spread(0)
    pair(1).wait()
    scalars.wait()
    both = sc[...] + sccame[...]
    for r in range(2):
        send[1, pl.ds(6 + r, CHIPS, stride=8), :] = jnp.broadcast_to(both[r:r + 1], (CHIPS, 128))
    merge(1)
    spread(1)

    totals = []
    for half in range(2):
        whole = recv.at[half]
        pltpu.make_async_copy(whole, whole, in_sem.at[half]).wait()
        total = send[half, pl.ds(pl.multiple_of(8 * chip, 8), 8), :]
        for r in range(CHIPS - 1):
            total = total + recv[half, pl.ds(8 * r, 8), :]
        totals.append(total)
    for half in range(2):
        whole = recv.at[half]
        pltpu.make_async_copy(whole, whole, out_sem.at[half]).wait()
    own = it[pl.ds(4 * me, 4)]
    kept = nt[pl.ds(4 * me, 4), :].astype(f32)
    for i in range(3):
        sig = totals[1][6:7, i:i + 1]
        inf = totals[1][7:8, i:i + 1]
        root = jnp.sqrt(inf * (1.0 / BINS))
        for r in range(2):
            for h in range(2):
                t = 2 * r + h
                row = totals[h][2 * i + r:2 * i + r + 1]
                out[t, i:i + 1] = kept[t:t + 1] * own[t, i:i + 1] * row / root
        board[i:i + 1, 0:1] = sig / jnp.sqrt(inf)
        board[i:i + 1, 1:2] = root


def local(strain, valid, intersection, notch):
    one, two, turns = tables()
    strain = strain.reshape(18, 2, 512, 128).transpose(0, 2, 1, 3).reshape(18, 1024, 128)
    inter = intersection.reshape(3, 512, 128).transpose(1, 0, 2)
    out, board = pl.pallas_call(
        kernel,
        out_shape=(jax.ShapeDtypeStruct((4, 3, 128), f32), jax.ShapeDtypeStruct((3, 2), f32)),
        in_specs=[pl.BlockSpec(memory_space=pltpu.SMEM)] + [pl.BlockSpec(memory_space=pl.ANY)] * 6,
        out_specs=(pl.BlockSpec(memory_space=pltpu.VMEM), pl.BlockSpec(memory_space=pltpu.VMEM)),
        scratch_shapes=[
            pltpu.VMEM((18, 1024, 128), bf16),
            pltpu.VMEM((4, 512, 128), bf16),
            pltpu.VMEM((4, 512, 128), bf16),
            pltpu.VMEM((2, F, F), f32),
            pltpu.VMEM((512, 4, 128), f32),
            pltpu.VMEM((512, 128), jnp.int32),
            pltpu.VMEM((3, 2, 128, F), f32),
            pltpu.VMEM((18, 4, F, 128), bf16),
            pltpu.VMEM((2, 9 * ROWS, 512), f32),
            pltpu.VMEM((3, 2, 128, F), f32),
            pltpu.VMEM((2, 2, 3, 128, 128), f32),
            pltpu.VMEM((2, 3, 128, 128), f32),
            pltpu.VMEM((2, 8 * CHIPS, 128), f32),
            pltpu.VMEM((2, 8 * (CHIPS - 1), 128), f32),
            pltpu.VMEM((8, 128), f32),
            pltpu.VMEM((8, 128), f32),
            pltpu.SemaphoreType.DMA((5,)),
            pltpu.SemaphoreType.DMA((18,)),
            pltpu.SemaphoreType.DMA((6,)),
            pltpu.SemaphoreType.DMA((2,)),
            pltpu.SemaphoreType.DMA((2,)),
        ],
        compiler_params=pltpu.CompilerParams(
            collective_id=0, has_side_effects=True, vmem_limit_bytes=60 * 2**20),
    )(valid, strain, inter, notch.reshape(512, 128), jnp.asarray(one), jnp.asarray(two), jnp.asarray(turns))
    return out.transpose(1, 0, 2).reshape(3, 512), board


def solution(mesh):
    in_specs = (P(None, "seg", None, None, None), P("seg"), P(), P())
    return jax.shard_map(local, mesh=mesh, in_specs=in_specs, out_specs=(P(None, "seg"), P()), check_vma=False)
```

```python
import functools
import math

import jax
import jax.numpy as jnp
import numpy as np
from jax import lax
from jax.experimental import pallas as pl
from jax.experimental.pallas import tpu as pltpu
from jax.sharding import PartitionSpec as P

MESH = pl.DeviceIdType.MESH
F = 256
BINS = F * F
CHIPS = 64
PAIRS = ((0, 1), (0, 2), (1, 2))
ROWS = 64
GROUP = 3
f32, bf16 = jnp.float32, jnp.bfloat16


def tables():
    k = np.arange(F)
    angle = 2 * np.pi * ((k[:, None] * k[None, :]) % F) / F
    cos, sin = (t(angle).astype(bf16).astype(np.float32) for t in (np.cos, np.sin))
    s = np.arange(8)
    a_of = (8 * np.arange(32)[:, None] + (s // 2 + 4 * (s % 2))[None, :]).reshape(-1)
    one = np.zeros((2, F, F, 2), np.float32)
    one[0, :, :, 0], one[0, :, :, 1] = cos[:, a_of], sin[:, a_of]
    one[1, :, :, 0], one[1, :, :, 1] = -sin[:, a_of], cos[:, a_of]
    one = one.reshape(2, 16, 16, 512).transpose(1, 0, 2, 3).reshape(512, 512)
    one = one.reshape(512, 4, 128).transpose(1, 0, 2)
    w, r, chip = np.meshgrid(np.arange(2), np.arange(2), np.arange(CHIPS), indexing="ij")
    q_of = (4 * chip + 2 * w + r).reshape(-1)
    c, v = cos[:, q_of] / F, sin[:, q_of] / F
    two = np.block([[c, -v], [v, c]])
    two = two.reshape(512, 4, 128).transpose(1, 0, 2)
    turn = 2 * np.pi * (k[:, None] * k[None, :]) / BINS
    turns = np.stack([np.cos(turn), np.sin(turn)]).astype(np.float32)
    return one.astype(bf16), two.astype(bf16), turns


def kernel(valid, strain, inter, notch, one, two, turns, out,
           ok, x, l1, l2, uv, it, nt, at, mid, y, part, num, came, send, recv, sc, sccame,
           load_sem, x_sem, pair_sem, out_sem, in_sem):
    me = lax.axis_index("seg")
    chip, core = me // 2, lax.rem(me, 2)
    mate = me + 1 - 2 * core

    loads = [pltpu.make_async_copy(a, b, load_sem.at[n]) for n, (a, b) in enumerate(
        ((one, l1), (turns, uv), (two, l2), (inter, it.at[:, :3]), (notch, nt), (valid, ok)))]

    def take(k):
        part = pl.ds(k * GROUP, GROUP)
        return pltpu.make_async_copy(strain.at[part], x.at[part], x_sem.at[k])

    loads[0].start()
    take(0).start()
    loads[1].start()
    for k in range(1, 18 // GROUP):
        take(k).start()
    for c in loads[2:]:
        c.start()

    barrier = pltpu.get_barrier_semaphore()
    pl.semaphore_signal(barrier, inc=1, device_id=(mate,), device_id_type=MESH)

    @pl.loop(1, CHIPS)
    def _(r):
        to = lax.rem(chip + r, CHIPS) * 2 + core
        pl.semaphore_signal(barrier, inc=1, device_id=(to,), device_id_type=MESH)

    for r in range(2):
        send[0, pl.ds(6 + r, CHIPS, stride=8), :] = jnp.zeros((CHIPS, 128), f32)

    even = (lax.broadcasted_iota(jnp.int16, (16, 128), 0) & 2) == 0
    loads[0].wait()
    loads[1].wait()

    def one_transform(n):
        left, right = [], []
        for g in range(32):
            a, b = x[n, pl.ds(32 * g, 16), :], x[n, pl.ds(32 * g + 16, 16), :]
            left.append(jnp.where(even, a, pltpu.roll(b, 2, axis=0)))
            right.append(jnp.where(even, pltpu.roll(a, 14, axis=0), b))
        data = jnp.concatenate([jnp.concatenate(left, 0), jnp.concatenate(right, 0)], axis=1)
        table = jnp.concatenate([l1[k] for k in range(4)], axis=1)
        first = jnp.dot(table, data, preferred_element_type=f32)
        for g in range(16):
            re, im = first[32 * g:32 * g + 16], first[32 * g + 16:32 * g + 32]
            u, v = uv[0, pl.ds(16 * g, 16), :], uv[1, pl.ds(16 * g, 16), :]
            mr = (re * u + im * v).astype(bf16)
            mi = (im * u - re * v).astype(bf16)
            for h in range(2):
                mid[n, h, pl.ds(16 * g, 16), :] = mr[:, 128 * h:128 * h + 128]
                mid[n, 2 + h, pl.ds(16 * g, 16), :] = mi[:, 128 * h:128 * h + 128]

    @pl.loop(0, 18 // GROUP)
    def _(k):
        take(k).wait()
        for j in range(GROUP):
            one_transform(k * GROUP + j)

    loads[3].wait()
    loads[4].wait()
    rows4 = it.reshape(2048, 128)

    @pl.loop(0, 2)
    def _(h):
        for w in range(2):
            keep = [nt[pl.ds(2 * (2 * w + r) + h, CHIPS, stride=8), :].astype(f32) for r in range(2)]
            for i in range(3):
                got = [rows4[pl.ds(8 * (2 * w + r) + 4 * h + i, CHIPS, stride=32), :] * keep[r] for r in range(2)]
                at[i, h, :, w * 128:(w + 1) * 128] = jnp.concatenate(got, axis=0).T

    loads[2].wait()
    loads[5].wait()

    def second(block, s, slot):
        rows = pl.ds(pl.multiple_of(ROWS * block, ROWS), ROWS)
        which = [d * 6 + s * 3 + t for t in range(3) for d in range(3)]
        data = jnp.concatenate(
            [jnp.concatenate([mid[n, k, rows, :] for n in which], axis=0) for k in range(4)], axis=1)
        table = jnp.concatenate([l2[k] for k in range(4)], axis=1)
        y[slot] = jnp.dot(data, table, preferred_element_type=f32)

    zero = (jnp.zeros((8, 128), f32),) * 3

    def stats(block, s, slot, signal, info):
        signal, info = list(signal), list(info)
        flag = ok[s].astype(f32)
        for g in range(ROWS // 8):
            for w in range(2):
                lane = slice(128 * w, 128 * w + 128)
                lane_im = slice(256 + 128 * w, 384 + 128 * w)
                power = [None] * 3
                cross = [None] * 3
                for t in range(3):
                    at_row = lambda d: pl.ds(ROWS * (3 * t + d) + 8 * g, 8)
                    re = [y[slot, at_row(d), lane] for d in range(3)]
                    im = [y[slot, at_row(d), lane_im] for d in range(3)]
                    for d in range(3):
                        v = re[d] * re[d] + im[d] * im[d]
                        power[d] = v if t == 0 else power[d] + v
                    for i, (a, b) in enumerate(PAIRS):
                        v = re[a] * re[b] + im[a] * im[b]
                        cross[i] = v if t == 0 else cross[i] + v
                third = [p * (1.0 / 3.0) for p in power]
                half, row = block // 2, ROWS * (block % 2) + 8 * g
                row = pl.ds(row if isinstance(row, int) else pl.multiple_of(row, 8), 8)
                for i, (a, b) in enumerate(PAIRS):
                    weight = flag / (third[a] * third[b])
                    v = weight * (cross[i] * (1.0 / 3.0))
                    f = at[i, half, row, lane]
                    signal[i] = signal[i] + f * v
                    info[i] = info[i] + f * f * weight
                    if s == 0:
                        part[i, half, row, lane] = v
                    else:
                        part[i, half, row, lane] = part[i, half, row, lane] + v
        return tuple(signal), tuple(info)

    def pair(half):
        return pltpu.make_async_remote_copy(
            src_ref=num.at[half, 1 - core], dst_ref=came.at[half],
            send_sem=pair_sem.at[half], recv_sem=pair_sem.at[2 + half],
            device_id=(mate,), device_id_type=MESH)

    def turn(half):
        for w in range(2):
            for i in range(3):
                num[half, w, i] = part[i, half, :, w * 128:(w + 1) * 128].T

    def merge(half):
        for i in range(3):
            for r in range(2):
                send[half, pl.ds(2 * i + r, CHIPS, stride=8), :] = (
                    num[half, core, i, pl.ds(CHIPS * r, CHIPS), :] + came[half, i, pl.ds(CHIPS * r, CHIPS), :])

    def spread(half):
        @pl.loop(1, CHIPS)
        def _(r):
            to = lax.rem(chip + r, CHIPS)
            pltpu.make_async_remote_copy(
                src_ref=send.at[half, pl.ds(pl.multiple_of(8 * to, 8), 8)],
                dst_ref=recv.at[half, pl.ds(pl.multiple_of(8 * (r - 1), 8), 8)],
                send_sem=out_sem.at[half], recv_sem=in_sem.at[half],
                device_id=(2 * to + core,), device_id_type=MESH).start()

    second(0, 0, 0)

    def step(block, sums):
        second(block, 1, 1)
        sums = stats(block, 0, 0, *sums)
        second(block + 1, 0, 0)
        sums = stats(block, 1, 1, *sums)

        @pl.when(block == 1)
        def _():
            turn(0)
            pl.semaphore_wait(barrier, CHIPS)
            pair(0).start()

        @pl.when(block == 2)
        def _():
            pair(0).wait()
            merge(0)
            spread(0)

        return sums

    sums = lax.fori_loop(0, F // ROWS - 1, step, (zero, zero))
    last = F // ROWS - 1
    second(last, 1, 1)
    sums = stats(last, 0, 0, *sums)
    sums = stats(last, 1, 1, *sums)
    signal, info = map(list, sums)
    turn(1)
    rows = [jnp.sum(a, axis=0, keepdims=True) for a in signal + info]
    cells = [jnp.sum(a, axis=1, keepdims=True) for a in rows]
    lanes = lax.broadcasted_iota(jnp.int32, (1, 128), 1)
    lines = []
    for group in (cells[:3], cells[3:]):
        line = jnp.zeros((1, 128), f32)
        for i in range(3):
            line = jnp.where(lanes == i, group[i], line)
        lines.append(line)
    sc[...] = jnp.concatenate(lines + [jnp.zeros((6, 128), f32)], axis=0)
    scalars = pltpu.make_async_remote_copy(
        src_ref=sc, dst_ref=sccame, send_sem=pair_sem.at[4], recv_sem=pair_sem.at[5],
        device_id=(mate,), device_id_type=MESH)
    pair(1).start()
    scalars.start()
    pair(1).wait()
    scalars.wait()
    both = sc[...] + sccame[...]
    for r in range(2):
        send[1, pl.ds(6 + r, CHIPS, stride=8), :] = jnp.broadcast_to(both[r:r + 1], (CHIPS, 128))
    merge(1)
    spread(1)

    totals = []
    for half in range(2):
        whole = recv.at[half]
        pltpu.make_async_copy(whole, whole, in_sem.at[half]).wait()
        total = send[half, pl.ds(pl.multiple_of(8 * chip, 8), 8), :]
        for r in range(CHIPS - 1):
            total = total + recv[half, pl.ds(8 * r, 8), :]
        totals.append(total)
    for half in range(2):
        whole = recv.at[half]
        pltpu.make_async_copy(whole, whole, out_sem.at[half]).wait()
    own = it[pl.ds(4 * me, 4)]
    kept = nt[pl.ds(4 * me, 4), :].astype(f32)
    for i in range(3):
        sig = totals[1][6:7, i:i + 1]
        inf = totals[1][7:8, i:i + 1]
        root = jnp.sqrt(inf * (1.0 / BINS))
        for r in range(2):
            for h in range(2):
                t = 2 * r + h
                row = totals[h][2 * i + r:2 * i + r + 1]
                out[t, i:i + 1] = kept[t:t + 1] * own[t, i:i + 1] * row / root
        out[4, 0:1, i:i + 1] = sig / jnp.sqrt(inf)
        out[4, 1:2, i:i + 1] = root


def hand_on(result, out, board):
    out[...] = result[0:4]
    board[...] = result[4, 0:2, 0:3]


def local(strain, valid, intersection, notch):
    one, two, turns = tables()
    strain = strain.reshape(18, 2, 512, 128).transpose(0, 2, 1, 3).reshape(18, 1024, 128)
    inter = intersection.reshape(3, 512, 128).transpose(1, 0, 2)
    result = pl.pallas_call(
        kernel,
        out_shape=jax.ShapeDtypeStruct((5, 3, 128), f32),
        in_specs=[pl.BlockSpec(memory_space=pl.ANY)] * 7,
        out_specs=pl.BlockSpec(memory_space=pltpu.VMEM),
        scratch_shapes=[
            pltpu.SMEM((2,), jnp.int32),
            pltpu.VMEM((18, 1024, 128), bf16),
            pltpu.VMEM((4, 512, 128), bf16),
            pltpu.VMEM((4, 512, 128), bf16),
            pltpu.VMEM((2, F, F), f32),
            pltpu.VMEM((512, 4, 128), f32),
            pltpu.VMEM((512, 128), jnp.int32),
            pltpu.VMEM((3, 2, 128, F), f32),
            pltpu.VMEM((18, 4, F, 128), bf16),
            pltpu.VMEM((2, 9 * ROWS, 512), f32),
            pltpu.VMEM((3, 2, 128, F), f32),
            pltpu.VMEM((2, 2, 3, 128, 128), f32),
            pltpu.VMEM((2, 3, 128, 128), f32),
            pltpu.VMEM((2, 8 * CHIPS, 128), f32),
            pltpu.VMEM((2, 8 * (CHIPS - 1), 128), f32),
            pltpu.VMEM((8, 128), f32),
            pltpu.VMEM((8, 128), f32),
            pltpu.SemaphoreType.DMA((6,)),
            pltpu.SemaphoreType.DMA((18,)),
            pltpu.SemaphoreType.DMA((6,)),
            pltpu.SemaphoreType.DMA((2,)),
            pltpu.SemaphoreType.DMA((2,)),
        ],
        compiler_params=pltpu.CompilerParams(
            collective_id=0, has_side_effects=True, vmem_limit_bytes=40*2**20),
    )(*(pltpu.with_memory_space_constraint(a, pltpu.HBM) for a in (valid, strain, inter, notch.reshape(512, 128), jnp.asarray(one), jnp.asarray(two), jnp.asarray(turns))))
    out, board = pl.pallas_call(
        hand_on,
        out_shape=(jax.ShapeDtypeStruct((4, 3, 128), f32), jax.ShapeDtypeStruct((2, 3), f32)),
        in_specs=[pl.BlockSpec(memory_space=pltpu.VMEM)],
        out_specs=(pl.BlockSpec(memory_space=pltpu.VMEM), pl.BlockSpec(memory_space=pltpu.VMEM)),
        compiler_params=pltpu.CompilerParams(vmem_limit_bytes=2**20),
    )(result)
    return out.transpose(1, 0, 2).reshape(3, 512), board.T


def solution(mesh):
    in_specs = (P(None, "seg", None, None, None), P("seg"), P(), P())
    return jax.shard_map(local, mesh=mesh, in_specs=in_specs, out_specs=(P(None, "seg"), P()), check_vma=False)
```

```python
import functools
import math

import jax
import jax.numpy as jnp
import numpy as np
from jax import lax
from jax.experimental import pallas as pl
from jax.experimental.pallas import tpu as pltpu
from jax.sharding import PartitionSpec as P

MESH = pl.DeviceIdType.MESH
F = 256
BINS = F * F
CHIPS = 64
PAIRS = ((0, 1), (0, 2), (1, 2))
ROWS = 64
GROUP = 3
STATIC = 2
ORDER = sorted(range(1, CHIPS), key=lambda n: -sum((0, 1, 2, 1)[n // k % 4] for k in (1, 4, 16)))
f32, bf16 = jnp.float32, jnp.bfloat16


def tables():
    k = np.arange(F)
    angle = 2 * np.pi * ((k[:, None] * k[None, :]) % F) / F
    cos, sin = (t(angle).astype(bf16).astype(np.float32) for t in (np.cos, np.sin))
    s = np.arange(8)
    a_of = (8 * np.arange(32)[:, None] + (s // 2 + 4 * (s % 2))[None, :]).reshape(-1)
    one = np.zeros((2, F, F, 2), np.float32)
    one[0, :, :, 0], one[0, :, :, 1] = cos[:, a_of], sin[:, a_of]
    one[1, :, :, 0], one[1, :, :, 1] = -sin[:, a_of], cos[:, a_of]
    one = one.reshape(2, 16, 16, 512).transpose(1, 0, 2, 3).reshape(512, 512)
    one = one.reshape(512, 4, 128).transpose(1, 0, 2)
    w, r, chip = np.meshgrid(np.arange(2), np.arange(2), np.arange(CHIPS), indexing="ij")
    q_of = (4 * chip + 2 * w + r).reshape(-1)
    c, v = cos[:, q_of] / F, sin[:, q_of] / F
    two = np.block([[c, -v], [v, c]])
    two = two.reshape(512, 4, 128).transpose(1, 0, 2)
    turn = 2 * np.pi * (k[:, None] * k[None, :]) / BINS
    turns = np.stack([np.cos(turn), np.sin(turn)]).astype(np.float32)
    return one.astype(bf16), two.astype(bf16), turns


def kernel(valid, strain, inter, notch, one, two, turns, out,
           ok, x, l1, l2, uv, it, nt, at, mid, y, part, num, came, send, recv, sc, sccame,
           load_sem, x_sem, pair_sem, out_sem, in_sem):
    me = lax.axis_index("seg")
    chip, core = me // 2, lax.rem(me, 2)
    mate = me + 1 - 2 * core

    loads = [pltpu.make_async_copy(a, b, load_sem.at[n]) for n, (a, b) in enumerate(
        ((one, l1), (turns, uv), (two, l2), (inter, it.at[:, :3]), (notch, nt), (valid, ok)))]

    def take(k):
        part = pl.ds(k * GROUP, GROUP)
        return pltpu.make_async_copy(strain.at[part], x.at[part], x_sem.at[k])

    loads[0].start()
    take(0).start()
    loads[1].start()
    for k in range(1, 18 // GROUP):
        take(k).start()
    for c in loads[2:]:
        c.start()

    barrier = pltpu.get_barrier_semaphore()
    pl.semaphore_signal(barrier, inc=1, device_id=(mate,), device_id_type=MESH)

    @pl.loop(1, CHIPS)
    def _(r):
        to = lax.rem(chip + r, CHIPS) * 2 + core
        pl.semaphore_signal(barrier, inc=1, device_id=(to,), device_id_type=MESH)

    for r in range(2):
        send[0, pl.ds(6 + r, CHIPS, stride=8), :] = jnp.zeros((CHIPS, 128), f32)

    even = (lax.broadcasted_iota(jnp.int16, (16, 128), 0) & 2) == 0
    loads[0].wait()
    loads[1].wait()

    def one_transform(n):
        left, right = [], []
        for g in range(32):
            a, b = x[n, pl.ds(32 * g, 16), :], x[n, pl.ds(32 * g + 16, 16), :]
            left.append(jnp.where(even, a, pltpu.roll(b, 2, axis=0)))
            right.append(jnp.where(even, pltpu.roll(a, 14, axis=0), b))
        data = jnp.concatenate([jnp.concatenate(left, 0), jnp.concatenate(right, 0)], axis=1)
        table = jnp.concatenate([l1[k] for k in range(4)], axis=1)
        first = jnp.dot(table, data, preferred_element_type=f32)
        for g in range(16):
            re, im = first[32 * g:32 * g + 16], first[32 * g + 16:32 * g + 32]
            u, v = uv[0, pl.ds(16 * g, 16), :], uv[1, pl.ds(16 * g, 16), :]
            mr = (re * u + im * v).astype(bf16)
            mi = (im * u - re * v).astype(bf16)
            for h in range(2):
                mid[n, h, pl.ds(16 * g, 16), :] = mr[:, 128 * h:128 * h + 128]
                mid[n, 2 + h, pl.ds(16 * g, 16), :] = mi[:, 128 * h:128 * h + 128]

    @pl.loop(0, 18 // GROUP)
    def _(k):
        take(k).wait()
        for j in range(GROUP):
            one_transform(k * GROUP + j)

    loads[3].wait()
    loads[4].wait()
    rows4 = it.reshape(2048, 128)

    @pl.loop(0, 2)
    def _(h):
        for w in range(2):
            keep = [nt[pl.ds(2 * (2 * w + r) + h, CHIPS, stride=8), :].astype(f32) for r in range(2)]
            for i in range(3):
                got = [rows4[pl.ds(8 * (2 * w + r) + 4 * h + i, CHIPS, stride=32), :] * keep[r] for r in range(2)]
                at[i, h, :, w * 128:(w + 1) * 128] = jnp.concatenate(got, axis=0).T

    loads[2].wait()
    loads[5].wait()

    def second(block, s, slot):
        rows = pl.ds(pl.multiple_of(ROWS * block, ROWS), ROWS)
        which = [d * 6 + s * 3 + t for t in range(3) for d in range(3)]
        data = jnp.concatenate(
            [jnp.concatenate([mid[n, k, rows, :] for n in which], axis=0) for k in range(4)], axis=1)
        table = jnp.concatenate([l2[k] for k in range(4)], axis=1)
        y[slot] = jnp.dot(data, table, preferred_element_type=f32)

    zero = (jnp.zeros((8, 128), f32),) * 3

    def stats(block, s, slot, info):
        info = list(info)
        flag = 3.0 * ok[s].astype(f32)
        for g in range(ROWS // 8):
            for w in range(2):
                lane = slice(128 * w, 128 * w + 128)
                lane_im = slice(256 + 128 * w, 384 + 128 * w)
                power = [None] * 3
                cross = [None] * 3
                for t in range(3):
                    at_row = lambda d: pl.ds(ROWS * (3 * t + d) + 8 * g, 8)
                    re = [y[slot, at_row(d), lane] for d in range(3)]
                    im = [y[slot, at_row(d), lane_im] for d in range(3)]
                    for d in range(3):
                        v = re[d] * re[d] + im[d] * im[d]
                        power[d] = v if t == 0 else power[d] + v
                    for i, (a, b) in enumerate(PAIRS):
                        v = re[a] * re[b] + im[a] * im[b]
                        cross[i] = v if t == 0 else cross[i] + v
                half, row = block // 2, ROWS * (block % 2) + 8 * g
                row = pl.ds(row if isinstance(row, int) else pl.multiple_of(row, 8), 8)
                for i, (a, b) in enumerate(PAIRS):
                    f = at[i, half, row, lane]
                    scaled = f * (flag / (power[a] * power[b]))
                    v = scaled * cross[i]
                    info[i] = info[i] + f * scaled
                    if s == 0:
                        part[i, half, row, lane] = v
                    else:
                        part[i, half, row, lane] = part[i, half, row, lane] + v
        return tuple(info)

    def pair(half):
        return pltpu.make_async_remote_copy(
            src_ref=num.at[half, 1 - core], dst_ref=came.at[half],
            send_sem=pair_sem.at[half], recv_sem=pair_sem.at[2 + half],
            device_id=(mate,), device_id_type=MESH)

    def turn(half, w):
        lane = pl.ds(pl.multiple_of(128 * w, 128), 128)
        for i in range(3):
            num[half, w, i] = part[i, half, :, lane].T

    def merge(half):
        for i in range(3):
            for r in range(2):
                send[half, pl.ds(2 * i + r, CHIPS, stride=8), :] = (
                    num[half, core, i, pl.ds(CHIPS * r, CHIPS), :] + came[half, i, pl.ds(CHIPS * r, CHIPS), :])

    z, across, up = lax.rem(chip, 4), lax.rem(chip // 4, 4), chip // 16
    places = [[lax.rem(v + k, 4) * size for k in range(4)] for v, size in ((z, 1), (across, 4), (up, 16))]

    def pass_on(half, to, slot):
        pltpu.make_async_remote_copy(
            src_ref=send.at[half, pl.ds(pl.multiple_of(8 * to, 8), 8)],
            dst_ref=recv.at[half, pl.ds(8 * slot if isinstance(slot, int) else pl.multiple_of(8 * slot, 8), 8)],
            send_sem=out_sem.at[half], recv_sem=in_sem.at[half],
            device_id=(2 * to + core,), device_id_type=MESH).start()

    def spread(half):
        if half == STATIC or STATIC == 2:
            for slot, far in enumerate(ORDER):
                pass_on(half, places[0][far % 4] + places[1][far // 4 % 4] + places[2][far // 16], slot)
            return

        @pl.loop(1, CHIPS)
        def _(r):
            pass_on(half, lax.rem(chip + r, CHIPS), r - 1)

    second(0, 0, 0)

    def step(block, sums):
        second(block, 1, 1)
        sums = stats(block, 0, 0, sums)
        second(block + 1, 0, 0)
        sums = stats(block, 1, 1, sums)

        @pl.when(block == 1)
        def _():
            turn(0, 1 - core)
            pl.semaphore_wait(barrier, CHIPS)
            pair(0).start()
            turn(0, core)

        return sums

    sums = lax.fori_loop(0, F // ROWS - 1, step, zero)
    last = F // ROWS - 1
    pair(0).wait()
    merge(0)
    spread(0)
    second(last, 1, 1)
    sums = stats(last, 0, 0, sums)
    sums = stats(last, 1, 1, sums)
    info = list(sums)
    turn(1, 1 - core)
    pair(1).start()
    turn(1, core)
    signal = []
    for i in range(3):
        total = zero[0]
        for half in range(2):
            for g in range(16):
                for w in range(2):
                    total = total + part[i, half, pl.ds(8 * g, 8), 128 * w:128 * w + 128]
        signal.append(total)
    rows = [jnp.sum(a, axis=0, keepdims=True) for a in signal + info]
    cells = [jnp.sum(a, axis=1, keepdims=True) for a in rows]
    lanes = lax.broadcasted_iota(jnp.int32, (1, 128), 1)
    lines = []
    for group in (cells[:3], cells[3:]):
        line = jnp.zeros((1, 128), f32)
        for i in range(3):
            line = jnp.where(lanes == i, group[i], line)
        lines.append(line)
    sc[...] = jnp.concatenate(lines + [jnp.zeros((6, 128), f32)], axis=0)
    scalars = pltpu.make_async_remote_copy(
        src_ref=sc, dst_ref=sccame, send_sem=pair_sem.at[4], recv_sem=pair_sem.at[5],
        device_id=(mate,), device_id_type=MESH)
    scalars.start()
    pair(1).wait()
    scalars.wait()
    both = sc[...] + sccame[...]
    for r in range(2):
        send[1, pl.ds(6 + r, CHIPS, stride=8), :] = jnp.broadcast_to(both[r:r + 1], (CHIPS, 128))
    merge(1)
    spread(1)

    totals = []
    for half in range(2):
        whole = recv.at[half]
        pltpu.make_async_copy(whole, whole, in_sem.at[half]).wait()
        total = send[half, pl.ds(pl.multiple_of(8 * chip, 8), 8), :]
        for r in range(CHIPS - 1):
            total = total + recv[half, pl.ds(8 * r, 8), :]
        totals.append(total)
    for half in range(2):
        whole = recv.at[half]
        pltpu.make_async_copy(whole, whole, out_sem.at[half]).wait()
    for i in range(3):
        sig = totals[1][6:7, i:i + 1]
        inf = 3.0 * totals[1][7:8, i:i + 1]
        root = jnp.sqrt(inf * (1.0 / BINS))
        for r in range(2):
            for h in range(2):
                out[2 * r + h, i:i + 1] = totals[h][2 * i + r:2 * i + r + 1] / root
        out[4, 0:1, i:i + 1] = sig / jnp.sqrt(inf)
        out[4, 1:2, i:i + 1] = root


def hand_on(result, out, board):
    out[...] = result[0:4]
    board[...] = result[4, 0:2, 0:3]


def local(strain, valid, intersection, notch):
    one, two, turns = tables()
    strain = strain.reshape(18, 2, 512, 128).transpose(0, 2, 1, 3).reshape(18, 1024, 128)
    inter = intersection.reshape(3, 512, 128).transpose(1, 0, 2)
    result = pl.pallas_call(
        kernel,
        out_shape=jax.ShapeDtypeStruct((5, 3, 128), f32),
        in_specs=[pl.BlockSpec(memory_space=pl.ANY)] * 7,
        out_specs=pl.BlockSpec(memory_space=pltpu.VMEM),
        scratch_shapes=[
            pltpu.SMEM((2,), jnp.int32),
            pltpu.VMEM((18, 1024, 128), bf16),
            pltpu.VMEM((4, 512, 128), bf16),
            pltpu.VMEM((4, 512, 128), bf16),
            pltpu.VMEM((2, F, F), f32),
            pltpu.VMEM((512, 4, 128), f32),
            pltpu.VMEM((512, 128), jnp.int32),
            pltpu.VMEM((3, 2, 128, F), f32),
            pltpu.VMEM((18, 4, F, 128), bf16),
            pltpu.VMEM((2, 9 * ROWS, 512), f32),
            pltpu.VMEM((3, 2, 128, F), f32),
            pltpu.VMEM((2, 2, 3, 128, 128), f32),
            pltpu.VMEM((2, 3, 128, 128), f32),
            pltpu.VMEM((2, 8 * CHIPS, 128), f32),
            pltpu.VMEM((2, 8 * (CHIPS - 1), 128), f32),
            pltpu.VMEM((8, 128), f32),
            pltpu.VMEM((8, 128), f32),
            pltpu.SemaphoreType.DMA((6,)),
            pltpu.SemaphoreType.DMA((18,)),
            pltpu.SemaphoreType.DMA((6,)),
            pltpu.SemaphoreType.DMA((2,)),
            pltpu.SemaphoreType.DMA((2,)),
        ],
        compiler_params=pltpu.CompilerParams(
            collective_id=0, has_side_effects=True, vmem_limit_bytes=40*2**20),
    )(*(pltpu.with_memory_space_constraint(a, pltpu.HBM) for a in (valid, strain, inter, notch.reshape(512, 128), jnp.asarray(one), jnp.asarray(two), jnp.asarray(turns))))
    out, board = pl.pallas_call(
        hand_on,
        out_shape=(jax.ShapeDtypeStruct((4, 3, 128), f32), jax.ShapeDtypeStruct((2, 3), f32)),
        in_specs=[pl.BlockSpec(memory_space=pltpu.VMEM)],
        out_specs=(pl.BlockSpec(memory_space=pltpu.VMEM), pl.BlockSpec(memory_space=pltpu.VMEM)),
        compiler_params=pltpu.CompilerParams(vmem_limit_bytes=2**20),
    )(result)
    return out.transpose(1, 0, 2).reshape(3, 512), board.T


def solution(mesh):
    in_specs = (P(None, "seg", None, None, None), P("seg"), P(), P())
    return jax.shard_map(local, mesh=mesh, in_specs=in_specs, out_specs=(P(None, "seg"), P()), check_vma=False)
```

```python
import functools
import math

import jax
import jax.numpy as jnp
import numpy as np
from jax import lax
from jax.experimental import pallas as pl
from jax.experimental.pallas import tpu as pltpu
from jax.sharding import PartitionSpec as P

MESH = pl.DeviceIdType.MESH
F = 256
BINS = F * F
CHIPS = 64
PAIRS = ((0, 1), (0, 2), (1, 2))
ROWS = 64
GROUP = 6
STATIC = 2
ORDER = sorted(range(1, CHIPS), key=lambda n: -sum((0, 1, 2, 1)[n // k % 4] for k in (1, 4, 16)))
f32, bf16 = jnp.float32, jnp.bfloat16


def tables():
    k = np.arange(F)
    angle = 2 * np.pi * ((k[:, None] * k[None, :]) % F) / F
    cos, sin = (t(angle).astype(bf16).astype(np.float32) for t in (np.cos, np.sin))
    s = np.arange(8)
    a_of = (8 * np.arange(32)[:, None] + (s // 2 + 4 * (s % 2))[None, :]).reshape(-1)
    one = np.zeros((2, F, F, 2), np.float32)
    one[0, :, :, 0], one[0, :, :, 1] = cos[:, a_of], sin[:, a_of]
    one[1, :, :, 0], one[1, :, :, 1] = -sin[:, a_of], cos[:, a_of]
    one = one.reshape(2, 16, 16, 512).transpose(1, 0, 2, 3).reshape(512, 512)
    one = one.reshape(512, 4, 128).transpose(1, 0, 2)
    w, r, chip = np.meshgrid(np.arange(2), np.arange(2), np.arange(CHIPS), indexing="ij")
    q_of = (4 * chip + 2 * w + r).reshape(-1)
    c, v = cos[:, q_of] / F, sin[:, q_of] / F
    two = np.block([[c, -v], [v, c]])
    two = two.reshape(512, 4, 128).transpose(1, 0, 2)
    turn = 2 * np.pi * (k[:, None] * k[None, :]) / BINS
    turns = np.stack([np.cos(turn), np.sin(turn)]).astype(np.float32)
    return one.astype(bf16), two.astype(bf16), turns


def kernel(valid, strain, inter, notch, one, two, turns, out,
           ok, x, l1, l2, uv, it, nt, at, mid, y, part, num, came, send, recv, sc, sccame,
           load_sem, x_sem, pair_sem, out_sem, in_sem):
    me = lax.axis_index("seg")
    chip, core = me // 2, lax.rem(me, 2)
    mate = me + 1 - 2 * core

    loads = [pltpu.make_async_copy(a, b, load_sem.at[n]) for n, (a, b) in enumerate(
        ((one, l1), (turns, uv), (two, l2), (inter, it.at[:, :3]), (notch, nt), (valid, ok)))]

    def take(k):
        part = pl.ds(k * GROUP, GROUP)
        return pltpu.make_async_copy(strain.at[part], x.at[part], x_sem.at[k])

    loads[0].start()
    take(0).start()
    loads[1].start()
    for k in range(1, 18 // GROUP):
        take(k).start()
    for c in loads[2:]:
        c.start()

    barrier = pltpu.get_barrier_semaphore()
    pl.semaphore_signal(barrier, inc=1, device_id=(mate,), device_id_type=MESH)

    @pl.loop(1, CHIPS)
    def _(r):
        to = lax.rem(chip + r, CHIPS) * 2 + core
        pl.semaphore_signal(barrier, inc=1, device_id=(to,), device_id_type=MESH)

    for r in range(2):
        send[0, pl.ds(6 + r, CHIPS, stride=8), :] = jnp.zeros((CHIPS, 128), f32)

    even = (lax.broadcasted_iota(jnp.int16, (16, 128), 0) & 2) == 0
    loads[0].wait()
    loads[1].wait()

    def one_transform(n):
        left, right = [], []
        for g in range(32):
            a, b = x[n, pl.ds(32 * g, 16), :], x[n, pl.ds(32 * g + 16, 16), :]
            left.append(jnp.where(even, a, pltpu.roll(b, 2, axis=0)))
            right.append(jnp.where(even, pltpu.roll(a, 14, axis=0), b))
        data = jnp.concatenate([jnp.concatenate(left, 0), jnp.concatenate(right, 0)], axis=1)
        table = jnp.concatenate([l1[k] for k in range(4)], axis=1)
        first = jnp.dot(table, data, preferred_element_type=f32)
        for g in range(16):
            re, im = first[32 * g:32 * g + 16], first[32 * g + 16:32 * g + 32]
            u, v = uv[0, pl.ds(16 * g, 16), :], uv[1, pl.ds(16 * g, 16), :]
            mr = (re * u + im * v).astype(bf16)
            mi = (im * u - re * v).astype(bf16)
            for h in range(2):
                mid[n, h, pl.ds(16 * g, 16), :] = mr[:, 128 * h:128 * h + 128]
                mid[n, 2 + h, pl.ds(16 * g, 16), :] = mi[:, 128 * h:128 * h + 128]

    @pl.loop(0, 18 // GROUP)
    def _(k):
        take(k).wait()
        for j in range(GROUP):
            one_transform(k * GROUP + j)

    loads[3].wait()
    loads[4].wait()
    rows4 = it.reshape(2048, 128)

    @pl.loop(0, 2)
    def _(h):
        for w in range(2):
            keep = [nt[pl.ds(2 * (2 * w + r) + h, CHIPS, stride=8), :].astype(f32) for r in range(2)]
            for i in range(3):
                got = [rows4[pl.ds(8 * (2 * w + r) + 4 * h + i, CHIPS, stride=32), :] * keep[r] for r in range(2)]
                at[i, h, :, w * 128:(w + 1) * 128] = jnp.concatenate(got, axis=0).T

    loads[2].wait()
    loads[5].wait()

    def second(block, s, slot):
        rows = pl.ds(pl.multiple_of(ROWS * block, ROWS), ROWS)
        which = [d * 6 + s * 3 + t for t in range(3) for d in range(3)]
        data = jnp.concatenate(
            [jnp.concatenate([mid[n, k, rows, :] for n in which], axis=0) for k in range(4)], axis=1)
        table = jnp.concatenate([l2[k] for k in range(4)], axis=1)
        y[slot] = jnp.dot(data, table, preferred_element_type=f32)

    zero = (jnp.zeros((8, 128), f32),) * 3

    def stats(block, s, slot, info):
        info = list(info)
        flag = 3.0 * ok[s].astype(f32)
        for g in range(ROWS // 8):
            for w in range(2):
                lane = slice(128 * w, 128 * w + 128)
                lane_im = slice(256 + 128 * w, 384 + 128 * w)
                power = [None] * 3
                cross = [None] * 3
                for t in range(3):
                    at_row = lambda d: pl.ds(ROWS * (3 * t + d) + 8 * g, 8)
                    re = [y[slot, at_row(d), lane] for d in range(3)]
                    im = [y[slot, at_row(d), lane_im] for d in range(3)]
                    for d in range(3):
                        v = re[d] * re[d] + im[d] * im[d]
                        power[d] = v if t == 0 else power[d] + v
                    for i, (a, b) in enumerate(PAIRS):
                        v = re[a] * re[b] + im[a] * im[b]
                        cross[i] = v if t == 0 else cross[i] + v
                half, row = block // (128 // ROWS), ROWS * (block % (128 // ROWS)) + 8 * g
                row = pl.ds(row if isinstance(row, int) else pl.multiple_of(row, 8), 8)
                for i, (a, b) in enumerate(PAIRS):
                    f = at[i, half, row, lane]
                    scaled = f * (flag / (power[a] * power[b]))
                    v = scaled * cross[i]
                    info[i] = info[i] + f * scaled
                    if s == 0:
                        part[i, half, row, lane] = v
                    else:
                        part[i, half, row, lane] = part[i, half, row, lane] + v
        return tuple(info)

    def pair(half, i):
        return pltpu.make_async_remote_copy(
            src_ref=num.at[half, 1 - core, i], dst_ref=came.at[half, i],
            send_sem=pair_sem.at[3 * half + i], recv_sem=pair_sem.at[6 + 3 * half + i],
            device_id=(mate,), device_id_type=MESH)

    def turn(half, w, send_on=False):
        lane = pl.ds(pl.multiple_of(128 * w, 128), 128)
        for i in range(3):
            num[half, w, i] = part[i, half, :, lane].T
            if send_on:
                pair(half, i).start()

    def merge(half):
        for i in range(3):
            pair(half, i).wait()
            for r in range(2):
                send[half, pl.ds(2 * i + r, CHIPS, stride=8), :] = (
                    num[half, core, i, pl.ds(CHIPS * r, CHIPS), :] + came[half, i, pl.ds(CHIPS * r, CHIPS), :])

    z, across, up = lax.rem(chip, 4), lax.rem(chip // 4, 4), chip // 16
    places = [[lax.rem(v + k, 4) * size for k in range(4)] for v, size in ((z, 1), (across, 4), (up, 16))]

    def pass_on(half, to, slot):
        pltpu.make_async_remote_copy(
            src_ref=send.at[half, pl.ds(pl.multiple_of(8 * to, 8), 8)],
            dst_ref=recv.at[half, pl.ds(8 * slot if isinstance(slot, int) else pl.multiple_of(8 * slot, 8), 8)],
            send_sem=out_sem.at[half], recv_sem=in_sem.at[half],
            device_id=(2 * to + core,), device_id_type=MESH).start()

    def spread(half):
        if half == STATIC or STATIC == 2:
            for slot, far in enumerate(ORDER):
                pass_on(half, places[0][far % 4] + places[1][far // 4 % 4] + places[2][far // 16], slot)
            return

        @pl.loop(1, CHIPS)
        def _(r):
            pass_on(half, lax.rem(chip + r, CHIPS), r - 1)

    second(0, 0, 0)

    def step(block, sums):
        second(block, 1, 1)
        sums = stats(block, 0, 0, sums)
        second(block + 1, 0, 0)
        sums = stats(block, 1, 1, sums)

        @pl.when(block == 128 // ROWS - 1)
        def _():
            pl.semaphore_wait(barrier, CHIPS)
            turn(0, 1 - core, True)
            turn(0, core)

        return sums

    sums = lax.fori_loop(0, F // ROWS - 1, step, zero)
    last = F // ROWS - 1
    merge(0)
    spread(0)
    second(last, 1, 1)
    sums = stats(last, 0, 0, sums)
    sums = stats(last, 1, 1, sums)
    info = list(sums)
    turn(1, 1 - core, True)
    turn(1, core)
    signal = []
    for i in range(3):
        total = zero[0]
        for half in range(2):
            for g in range(16):
                for w in range(2):
                    total = total + part[i, half, pl.ds(8 * g, 8), 128 * w:128 * w + 128]
        signal.append(total)
    rows = [jnp.sum(a, axis=0, keepdims=True) for a in signal + info]
    cells = [jnp.sum(a, axis=1, keepdims=True) for a in rows]
    lanes = lax.broadcasted_iota(jnp.int32, (1, 128), 1)
    lines = []
    for group in (cells[:3], cells[3:]):
        line = jnp.zeros((1, 128), f32)
        for i in range(3):
            line = jnp.where(lanes == i, group[i], line)
        lines.append(line)
    sc[...] = jnp.concatenate(lines + [jnp.zeros((6, 128), f32)], axis=0)
    scalars = pltpu.make_async_remote_copy(
        src_ref=sc, dst_ref=sccame, send_sem=pair_sem.at[12], recv_sem=pair_sem.at[13],
        device_id=(mate,), device_id_type=MESH)
    scalars.start()
    scalars.wait()
    both = sc[...] + sccame[...]
    for r in range(2):
        send[1, pl.ds(6 + r, CHIPS, stride=8), :] = jnp.broadcast_to(both[r:r + 1], (CHIPS, 128))
    merge(1)
    spread(1)

    totals = []
    for half in range(2):
        whole = recv.at[half]
        pltpu.make_async_copy(whole, whole, in_sem.at[half]).wait()
        total = send[half, pl.ds(pl.multiple_of(8 * chip, 8), 8), :]
        for r in range(CHIPS - 1):
            total = total + recv[half, pl.ds(8 * r, 8), :]
        totals.append(total)
    for half in range(2):
        whole = recv.at[half]
        pltpu.make_async_copy(whole, whole, out_sem.at[half]).wait()
    for i in range(3):
        sig = totals[1][6:7, i:i + 1]
        inf = 3.0 * totals[1][7:8, i:i + 1]
        root = jnp.sqrt(inf * (1.0 / BINS))
        for r in range(2):
            for h in range(2):
                out[2 * r + h, i:i + 1] = totals[h][2 * i + r:2 * i + r + 1] / root
        out[4, 0:1, i:i + 1] = sig / jnp.sqrt(inf)
        out[4, 1:2, i:i + 1] = root


def hand_on(result, out, board):
    out[...] = result[0:4]
    board[...] = result[4, 0:2, 0:3]


def local(strain, valid, intersection, notch):
    one, two, turns = tables()
    strain = strain.reshape(18, 2, 512, 128).transpose(0, 2, 1, 3).reshape(18, 1024, 128)
    inter = intersection.reshape(3, 512, 128).transpose(1, 0, 2)
    result = pl.pallas_call(
        kernel,
        out_shape=jax.ShapeDtypeStruct((5, 3, 128), f32),
        in_specs=[pl.BlockSpec(memory_space=pl.ANY)] * 7,
        out_specs=pl.BlockSpec(memory_space=pltpu.VMEM),
        scratch_shapes=[
            pltpu.SMEM((2,), jnp.int32),
            pltpu.VMEM((18, 1024, 128), bf16),
            pltpu.VMEM((4, 512, 128), bf16),
            pltpu.VMEM((4, 512, 128), bf16),
            pltpu.VMEM((2, F, F), f32),
            pltpu.VMEM((512, 4, 128), f32),
            pltpu.VMEM((512, 128), jnp.int32),
            pltpu.VMEM((3, 2, 128, F), f32),
            pltpu.VMEM((18, 4, F, 128), bf16),
            pltpu.VMEM((2, 9 * ROWS, 512), f32),
            pltpu.VMEM((3, 2, 128, F), f32),
            pltpu.VMEM((2, 2, 3, 128, 128), f32),
            pltpu.VMEM((2, 3, 128, 128), f32),
            pltpu.VMEM((2, 8 * CHIPS, 128), f32),
            pltpu.VMEM((2, 8 * (CHIPS - 1), 128), f32),
            pltpu.VMEM((8, 128), f32),
            pltpu.VMEM((8, 128), f32),
            pltpu.SemaphoreType.DMA((6,)),
            pltpu.SemaphoreType.DMA((18,)),
            pltpu.SemaphoreType.DMA((14,)),
            pltpu.SemaphoreType.DMA((2,)),
            pltpu.SemaphoreType.DMA((2,)),
        ],
        compiler_params=pltpu.CompilerParams(
            collective_id=0, has_side_effects=True, vmem_limit_bytes=40*2**20),
    )(*(pltpu.with_memory_space_constraint(a, pltpu.HBM) for a in (valid, strain, inter, notch.reshape(512, 128), jnp.asarray(one), jnp.asarray(two), jnp.asarray(turns))))
    out, board = pl.pallas_call(
        hand_on,
        out_shape=(jax.ShapeDtypeStruct((4, 3, 128), f32), jax.ShapeDtypeStruct((2, 3), f32)),
        in_specs=[pl.BlockSpec(memory_space=pltpu.VMEM)],
        out_specs=(pl.BlockSpec(memory_space=pltpu.VMEM), pl.BlockSpec(memory_space=pltpu.VMEM)),
        compiler_params=pltpu.CompilerParams(vmem_limit_bytes=2**20),
    )(result)
    return out.transpose(1, 0, 2).reshape(3, 512), board.T


def solution(mesh):
    in_specs = (P(None, "seg", None, None, None), P("seg"), P(), P())
    return jax.shard_map(local, mesh=mesh, in_specs=in_specs, out_specs=(P(None, "seg"), P()), check_vma=False)
```
